32 devices in a mesh: rep: 1 (over z), dp: 32 (over x, y, core).
Axes of the slice: x: 4, y: 4, z: 1, core: 2. Of those that a mesh axis runs over, the one named last changes fastest.
The devices are a block of a 4x4x8 slice.
Arguments:
- a: bfloat16 [32, 2, 4096, 1024], P(('rep', 'dp'))
- g: bfloat16 [32, 2, 4096, 2560], P(('rep', 'dp'))
Outputs:
- output: bfloat16 [2, 1024, 2560], P('rep')
All inputs are finite; a program needn't handle non-finite values.
Results may differ from the reference program's by a relative error of at most 0.012.
Values are sent between devices in bfloat16 or wider.
A program may use at most 768 MiB of HBM per device.

```python
import jax
import jax.numpy as jnp
from jax import lax

DEVICES = 32
MATRICES = 2
TOKENS = 4096
D = 1024
FF = 2560


def setup_inputs(seed: int = 0, part: int = 0) -> dict:
    ka, kg, ks = (jax.random.fold_in(k, part) for k in jax.random.split(jax.random.key(seed), 3))
    size = 2.0 ** jax.random.uniform(ks, (DEVICES, MATRICES, 1, 1), jnp.float32, -1.0, 1.0)
    a = jax.random.normal(ka, (DEVICES, MATRICES, TOKENS, D), jnp.float32)
    g = size * jax.random.normal(kg, (DEVICES, MATRICES, TOKENS, FF), jnp.float32) * (DEVICES * TOKENS) ** -0.5
    return {"a": a.astype(jnp.bfloat16), "g": g.astype(jnp.bfloat16)}


def reference(a, g):
    def take(so_far, one):
        return so_far + jnp.einsum("ntd,ntf->ndf", *one, preferred_element_type=jnp.float32), None

    return lax.scan(take, jnp.zeros((MATRICES, D, FF), jnp.float32), (a, g))[0].astype(jnp.bfloat16)
```

```python
import functools
import math

import jax
import jax.numpy as jnp
from jax import lax
from jax.experimental import pallas as pl
from jax.experimental.pallas import tpu as pltpu
from jax.sharding import PartitionSpec as P

CORES = 2
RING = 4
SLOTS = 3
MESSAGES = 25
MESH = pl.DeviceIdType.MESH


def kernel(
    pieces, width, a_hbm, g_hbm, out_hbm,
    a_buf, g_buf, own, pair_send, pair_recv, raw, mid1, sum1, mid2, recv1, recv2, res,
    a_sem, g_sem, out_sem, send_sem, recv_sem,
):
    matrices, tokens, d = a_hbm.shape[1:]
    half = d // CORES
    block = half // RING
    cell = block // RING
    per_matrix = pieces // matrices

    me = lax.axis_index("dp")
    core = lax.rem(me, CORES)
    chip = me // CORES
    x, y = chip // RING, lax.rem(chip, RING)
    other = 1 - core
    p1 = x * other + y * core
    p2 = y * other + x * core

    def at(q1, q2):
        return ((q1 * other + q2 * core) * RING + q2 * other + q1 * core) * CORES + core

    def step(p, by):
        return lax.rem(p + by + RING, RING)

    partner = chip * CORES + other
    right1, left1 = at(step(p1, 1), p2), at(step(p1, -1), p2)
    right2, left2 = at(p1, step(p2, 1)), at(p1, step(p2, -1))
    peers = (partner, right1, left1, right2, left2)

    def rows(start, size):
        return pl.ds(pl.multiple_of(start, size), size)

    def copy(j, message, src, dst, device):
        return pltpu.make_async_remote_copy(
            src_ref=src, dst_ref=dst, send_sem=send_sem.at[j, message], recv_sem=recv_sem.at[j, message],
            device_id={"dp": device}, device_id_type=MESH,
        )

    def send(j, message, src, dst, device):
        copy(j, message, src, dst, device).start()

    def sent(j, message, src):
        copy(j, message, src, src, partner).wait_send()

    def got(j, message, dst):
        copy(j, message, dst, dst, partner).wait_recv()

    def load_a(n, h):
        start = (core * h + other * (1 - h)) * half
        return pltpu.make_async_copy(
            a_hbm.at[0, n, :, pl.ds(pl.multiple_of(start, half), half)], a_buf.at[n, h], a_sem.at[n, h]
        )

    def load_g(j):
        n, c = j // per_matrix, lax.rem(j, per_matrix)
        s = lax.rem(j, SLOTS)
        return pltpu.make_async_copy(
            g_hbm.at[0, n, :, pl.ds(pl.multiple_of(c * width, width), width)], g_buf.at[s], g_sem.at[j]
        )

    def store_out(j):
        n, c = j // per_matrix, lax.rem(j, per_matrix)
        return pltpu.make_async_copy(
            res.at[j], out_hbm.at[n, :, pl.ds(pl.multiple_of(c * width, width), width)], out_sem.at[j]
        )

    def dot(j, h):
        n, s = j // per_matrix, lax.rem(j, SLOTS)
        return lax.dot_general(
            a_buf[n, h], g_buf[s], (((0,), (0,)), ((), ())), preferred_element_type=jnp.float32
        )

    load_a(0, 0).start()
    load_g(0).start()
    load_a(0, 1).start()
    load_g(1).start()
    load_g(2).start()
    for n in range(1, matrices):
        for h in range(2):
            load_a(n, h).start()

    barrier = pltpu.get_barrier_semaphore()
    for peer in peers:
        pl.semaphore_signal(barrier, inc=1, device_id={"dp": peer}, device_id_type=MESH)
    pl.semaphore_wait(barrier, len(peers))

    def partner_half(j):
        load_g(j).wait()

        @pl.when(lax.rem(j, per_matrix) == 0)
        def _():
            load_a(j // per_matrix, 0).wait()

        s = lax.rem(j, 2)
        pair_send[s] = dot(j, 0).astype(jnp.bfloat16)
        send(j, 0, pair_send.at[s], pair_recv.at[j], partner)

    def own_half(j):
        @pl.when(lax.rem(j, per_matrix) == 0)
        def _():
            load_a(j // per_matrix, 1).wait()

        s = lax.rem(j, SLOTS)
        got(j, 0, pair_recv.at[j])
        total = dot(j, 1) + pair_recv[j].astype(jnp.float32)
        own[s] = total
        raw[s] = total.astype(jnp.bfloat16)

        @pl.when(j + SLOTS < pieces)
        def _():
            load_g(j + SLOTS).start()

        scatter_raw(j, 1, raw.at[s], recv1.at[j], p1, block, right1, left1)
        sent(j, 0, pair_send.at[lax.rem(j, 2)])

    def scatter_raw(j, first, src, dst, p, size, right, left):
        h = size // 2
        far, near_r, near_l = step(p, 2) * size, step(p, 1) * size, step(p, -1) * size
        send(j, first, src.at[rows(far, h)], dst.at[0], right)
        send(j, first + 1, src.at[rows(far + h, h)], dst.at[1], left)
        send(j, first + 2, src.at[rows(near_r + h, h)], dst.at[2], right)
        send(j, first + 3, src.at[rows(near_l, h)], dst.at[3], left)

    def scatter_mid(j, first, acc, stage, dst, p, size, right, left):
        h = size // 2
        near_r, near_l = step(p, 1) * size, step(p, -1) * size
        got(j, first, dst.at[0])
        stage[0] = (acc[rows(near_r, h)] + dst[0].astype(jnp.float32)).astype(jnp.bfloat16)
        send(j, first + 4, stage.at[0], dst.at[4], right)
        got(j, first + 1, dst.at[1])
        stage[1] = (acc[rows(near_l + h, h)] + dst[1].astype(jnp.float32)).astype(jnp.bfloat16)
        send(j, first + 5, stage.at[1], dst.at[5], left)

    def scatter_sum(j, first, acc, dst, p, size):
        h = size // 2
        for m in (2, 3, 4, 5):
            got(j, first + m, dst.at[m])
        upper = acc[rows(p * size, h)] + (dst[3].astype(jnp.float32) + dst[4].astype(jnp.float32))
        lower = acc[rows(p * size + h, h)] + (dst[2].astype(jnp.float32) + dst[5].astype(jnp.float32))
        return upper, lower

    def scatter_sent(j, first, src, stage, size):
        h = size // 2
        for m in range(4):
            sent(j, first + m, src.at[pl.ds(0, h)])
        for m in range(2):
            sent(j, first + 4 + m, stage.at[m])

    def mid_1(j):
        s = lax.rem(j, SLOTS)
        scatter_mid(j, 1, own.at[s], mid1.at[s], recv1.at[j], p1, block, right1, left1)

    def sum_1(j):
        s = lax.rem(j, SLOTS)
        h = block // 2
        for part, value in enumerate(scatter_sum(j, 1, own.at[s], recv1.at[j], p1, block)):
            own[s, pl.ds(part * h, h)] = value
            sum1[s, pl.ds(part * h, h)] = value.astype(jnp.bfloat16)
        scatter_raw(j, 7, sum1.at[s], recv2.at[j], p2, cell, right2, left2)

    def mid_2(j):
        s = lax.rem(j, SLOTS)
        scatter_mid(j, 7, own.at[s], mid2.at[s], recv2.at[j], p2, cell, right2, left2)

    def cells(q1, q2):
        return core * half + q1 * block + q2 * cell

    def sum_2(j):
        s = lax.rem(j, SLOTS)
        h = cell // 2
        for part, value in enumerate(scatter_sum(j, 7, own.at[s], recv2.at[j], p2, cell)):
            res[j, rows(cells(p1, p2) + part * h, h)] = value.astype(jnp.bfloat16)
        mine = res.at[j, rows(cells(p1, p2), cell)]
        send(j, 13, mine, mine, right2)
        send(j, 14, mine, mine, left2)

    def piece_rows(j, start, size):
        return res.at[j, rows(start, size)]

    def gather_mid_2(j):
        h = cell // 2
        got(j, 13, piece_rows(j, cells(p1, step(p2, -1)), cell))
        ref = piece_rows(j, cells(p1, step(p2, -1)), h)
        send(j, 15, ref, ref, right2)
        got(j, 14, piece_rows(j, cells(p1, step(p2, 1)), cell))
        ref = piece_rows(j, cells(p1, step(p2, 1)) + h, h)
        send(j, 16, ref, ref, left2)
        scatter_sent(j, 1, raw.at[0], mid1.at[0], block)

    def gather_1(j):
        h = cell // 2
        got(j, 15, piece_rows(j, cells(p1, step(p2, 2)), h))
        got(j, 16, piece_rows(j, cells(p1, step(p2, 2)) + h, h))
        mine = piece_rows(j, cells(p1, 0), block)
        send(j, 17, mine, mine, right1)
        send(j, 18, mine, mine, left1)
        send(j, 21, mine, mine, partner)

    def gather_mid_1(j):
        h = block // 2
        from_left, from_right = cells(step(p1, -1), 0), cells(step(p1, 1), 0)
        got(j, 17, piece_rows(j, from_left, block))
        ref = piece_rows(j, from_left, h)
        send(j, 19, ref, ref, right1)
        got(j, 18, piece_rows(j, from_right, block))
        ref = piece_rows(j, from_right + h, h)
        send(j, 20, ref, ref, left1)
        for message, start in ((22, from_left), (23, from_right)):
            ref = piece_rows(j, start, block)
            send(j, message, ref, ref, partner)
        scatter_sent(j, 7, sum1.at[0], mid2.at[0], cell)

    def gather_end(j):
        h = block // 2
        far = cells(step(p1, 2), 0)
        got(j, 19, piece_rows(j, far, h))
        got(j, 20, piece_rows(j, far + h, h))
        ref = piece_rows(j, far, block)
        send(j, 24, ref, ref, partner)

    def finish(j):
        for message in (13, 14):
            sent(j, message, res.at[j, pl.ds(0, cell)])
        for message in (15, 16):
            sent(j, message, res.at[j, pl.ds(0, cell // 2)])
        for message in (17, 18, 21, 22, 23, 24):
            sent(j, message, res.at[j, pl.ds(0, block)])
        for message in (19, 20):
            sent(j, message, res.at[j, pl.ds(0, block // 2)])
        theirs = other * half
        for message, by in ((21, 0), (22, -1), (23, 1), (24, 2)):
            got(j, message, piece_rows(j, theirs + step(p2, by) * block, block))
        store_out(j).start()

    def when_piece(j, stage):
        @pl.when((j >= 0) & (j < pieces))
        def _():
            stage(j)

    def body(i, _):
        when_piece(i, partner_half)
        when_piece(i - 6, finish)
        when_piece(i - 5, gather_mid_1)
        when_piece(i - 4, gather_mid_2)
        when_piece(i - 3, mid_2)
        when_piece(i - 2, mid_1)
        when_piece(i - 1, own_half)
        when_piece(i - 5, gather_end)
        when_piece(i - 4, gather_1)
        when_piece(i - 3, sum_2)
        when_piece(i - 2, sum_1)
        return 0

    lax.fori_loop(0, pieces + 7, body, 0)
    lax.fori_loop(0, pieces, lambda j, _: (store_out(j).wait(), 0)[1], 0)


def solution(mesh):
    devices = mesh.shape["dp"]
    assert devices == CORES * RING * RING and RING == math.isqrt(devices // CORES)

    def sums(a, g):
        _, matrices, tokens, d = a.shape
        ff = g.shape[3]
        width = 512 if ff % 512 == 0 else 128
        pieces = matrices * ff // width
        half = d // CORES
        block, cell = half // RING, half // RING // RING
        bf16, f32 = jnp.bfloat16, jnp.float32
        return pl.pallas_call(
            functools.partial(kernel, pieces, width),
            out_shape=jax.ShapeDtypeStruct((matrices, d, ff), bf16),
            in_specs=[pl.BlockSpec(memory_space=pltpu.HBM)] * 2,
            out_specs=pl.BlockSpec(memory_space=pltpu.HBM),
            scratch_shapes=[
                pltpu.VMEM((matrices, 2, tokens, half), bf16),
                pltpu.VMEM((SLOTS, tokens, width), bf16),
                pltpu.VMEM((SLOTS, half, width), f32),
                pltpu.VMEM((2, half, width), bf16),
                pltpu.VMEM((pieces, half, width), bf16),
                pltpu.VMEM((SLOTS, half, width), bf16),
                pltpu.VMEM((SLOTS, 2, block // 2, width), bf16),
                pltpu.VMEM((SLOTS, block, width), bf16),
                pltpu.VMEM((SLOTS, 2, cell // 2, width), bf16),
                pltpu.VMEM((pieces, 6, block // 2, width), bf16),
                pltpu.VMEM((pieces, 6, cell // 2, width), bf16),
                pltpu.VMEM((pieces, d, width), bf16),
                pltpu.SemaphoreType.DMA((matrices, 2)),
                pltpu.SemaphoreType.DMA((pieces,)),
                pltpu.SemaphoreType.DMA((pieces,)),
                pltpu.SemaphoreType.DMA((pieces, MESSAGES)),
                pltpu.SemaphoreType.DMA((pieces, MESSAGES)),
            ],
            compiler_params=pltpu.CompilerParams(
                collective_id=0, has_side_effects=True, vmem_limit_bytes=63 * 2**20
            ),
        )(a, g)

    spec = P(("rep", "dp"))
    return jax.shard_map(sums, mesh=mesh, in_specs=(spec, spec), out_specs=P("rep"), check_vma=False)
```

```python
import functools
import math

import jax
import jax.numpy as jnp
from jax import lax
from jax.experimental import pallas as pl
from jax.experimental.pallas import tpu as pltpu
from jax.sharding import PartitionSpec as P

CORES = 2
RING = 4
MESSAGES = 25
VMEM_BYTES = 52 * 2**20
MESH = pl.DeviceIdType.MESH

DIRECT_FIRST, DIRECT_LAST = 2, 2
DIRECT = {"own_half": 3, "sum_1": 6, "sum_2": 8, "gather_1": 11, "gather_mid_1": 15, "gather_end": 16, "finish": 19}
PASSED = {"own_half": 3, "mid_1": 5, "sum_1": 8, "sum_2": 11, "gather_1": 14, "gather_mid_1": 16, "gather_end": 20, "finish": 23}


def slots(written, read):
    whens = [when for when in (DIRECT, PASSED) if written in when]
    return max((late[read] - early[written]) // 2 + 1 for late in whens for early in whens)


G_SLOTS = 3
OWN_SLOTS = slots("own_half", "sum_2")
RAW_SLOTS = slots("own_half", "sum_1")
MID_SLOTS = slots("mid_1", "sum_1")
SUM_SLOTS = slots("sum_1", "sum_2")


def kernel(
    pieces, width, a_hbm, g_hbm, res,
    a_buf, g_buf, own, pair_send, pair_recv, raw, mid1, sum1, recv1, recv2,
    a_sem, g_sem, send_sem, recv_sem,
):
    matrices, tokens, d = a_hbm.shape[1:]
    half = d // CORES
    block = half // RING
    cell = block // RING
    per_matrix = pieces // matrices

    me = lax.axis_index("dp")
    core = lax.rem(me, CORES)
    chip = me // CORES
    x, y = chip // RING, lax.rem(chip, RING)
    other = 1 - core
    p1 = x * other + y * core
    p2 = y * other + x * core

    def at(q1, q2):
        return ((q1 * other + q2 * core) * RING + q2 * other + q1 * core) * CORES + core

    def step(p, by):
        return lax.rem(p + by + RING, RING)

    partner = chip * CORES + other
    right1, left1, far1 = (at(step(p1, by), p2) for by in (1, -1, 2))
    right2, left2, far2 = (at(p1, step(p2, by)) for by in (1, -1, 2))
    peers = (partner, right1, left1, far1, right2, left2, far2)

    def rows(start, size):
        return pl.ds(pl.multiple_of(start, size), size)

    def copy(j, message, src, dst, device):
        return pltpu.make_async_remote_copy(
            src_ref=src, dst_ref=dst, send_sem=send_sem.at[j, message], recv_sem=recv_sem.at[j, message],
            device_id={"dp": device}, device_id_type=MESH,
        )

    def send(j, message, src, dst, device):
        copy(j, message, src, dst, device).start()

    def sent(j, message, src):
        copy(j, message, src, src, partner).wait_send()

    def got(j, message, dst):
        copy(j, message, dst, dst, partner).wait_recv()

    def load_a(n, h):
        start = (core * h + other * (1 - h)) * half
        return pltpu.make_async_copy(
            a_hbm.at[0, n, :, pl.ds(pl.multiple_of(start, half), half)], a_buf.at[n, h], a_sem.at[n, h]
        )

    def load_g(j):
        n, c = j // per_matrix, lax.rem(j, per_matrix)
        s = lax.rem(j, G_SLOTS)
        return pltpu.make_async_copy(
            g_hbm.at[0, n, :, pl.ds(pl.multiple_of(c * width, width), width)], g_buf.at[s], g_sem.at[j]
        )

    def dot(j, h):
        n, s = j // per_matrix, lax.rem(j, G_SLOTS)
        return lax.dot_general(
            a_buf[n, h], g_buf[s], (((0,), (0,)), ((), ())), preferred_element_type=jnp.float32
        )

    barrier = pltpu.get_barrier_semaphore()
    load_a(0, 0).start()
    load_g(0).start()
    for peer in peers:
        pl.semaphore_signal(barrier, inc=1, device_id={"dp": peer}, device_id_type=MESH)
    load_a(0, 1).start()
    load_g(1).start()
    load_g(2).start()

    def partner_dot(j):
        pair_send[lax.rem(j, 2)] = dot(j, 0).astype(jnp.bfloat16)

    def partner_send(j):
        send(j, 0, pair_send.at[lax.rem(j, 2)], pair_recv.at[j], partner)

    load_g(0).wait()
    load_a(0, 0).wait()
    partner_dot(0)
    pl.semaphore_wait(barrier, len(peers))
    partner_send(0)

    def partner_half(j):
        load_g(j).wait()

        @pl.when(lax.rem(j, per_matrix) == 0)
        def _():
            load_a(j // per_matrix, 0).wait()

        @pl.when((lax.rem(j, per_matrix) == 1) & (j // per_matrix + 1 < matrices))
        def _():
            for h in range(2):
                load_a(j // per_matrix + 1, h).start()

        partner_dot(j)
        partner_send(j)

    def direct(j):
        return (j < DIRECT_FIRST) | (j >= pieces - DIRECT_LAST)

    def either(j, if_direct, if_passed):
        pl.when(direct(j))(if_direct)
        pl.when(jnp.logical_not(direct(j)))(if_passed)

    def own_half(j):
        @pl.when(lax.rem(j, per_matrix) == 0)
        def _():
            load_a(j // per_matrix, 1).wait()

        s = lax.rem(j, RAW_SLOTS)
        got(j, 0, pair_recv.at[j])
        total = dot(j, 1) + pair_recv[j].astype(jnp.float32)
        own[lax.rem(j, OWN_SLOTS)] = total
        raw[s] = total.astype(jnp.bfloat16)

        @pl.when(j + G_SLOTS < pieces)
        def _():
            load_g(j + G_SLOTS).start()

        src, h = raw.at[s], block // 2
        far, near_r, near_l = (step(p1, by) * block for by in (2, 1, -1))

        def _direct():
            scatter(j, 1, src, recv1, p1, block, far1, right1, left1)

        def _passed():
            send(j, 1, src.at[rows(far, h)], recv1.at[j, pl.ds(0, h)], right1)
            send(j, 2, src.at[rows(far + h, h)], recv1.at[j, pl.ds(h, h)], left1)
            send(j, 3, src.at[rows(near_r + h, h)], recv1.at[j, pl.ds(2 * h, h)], right1)
            send(j, 4, src.at[rows(near_l, h)], recv1.at[j, pl.ds(3 * h, h)], left1)

        either(j, _direct, _passed)
        sent(j, 0, pair_send.at[lax.rem(j, 2)])

    def scatter(j, first, src, dst, p, size, far, right, left):
        for m, (by, device) in enumerate(((2, far), (1, right), (-1, left))):
            send(j, first + m, src.at[rows(step(p, by) * size, size)], dst.at[j, pl.ds(m * size, size)], device)

    def added(j, first, acc, dst, p, size):
        for m in range(3):
            got(j, first + m, dst.at[j, pl.ds(m * size, size)])
        far, left, right = (dst[j, pl.ds(m * size, size)].astype(jnp.float32) for m in range(3))
        return acc[rows(p * size, size)] + (left + right + far)

    def mid_1(j):
        s, h = lax.rem(j, MID_SLOTS), block // 2
        acc = own.at[lax.rem(j, OWN_SLOTS)]
        for m, device, start in ((0, right1, step(p1, 1) * block), (1, left1, step(p1, -1) * block + h)):
            got(j, 1 + m, recv1.at[j, pl.ds(m * h, h)])
            passed = acc[rows(start, h)] + recv1[j, pl.ds(m * h, h)].astype(jnp.float32)
            mid1[s, m] = passed.astype(jnp.bfloat16)
            send(j, 5 + m, mid1.at[s, m], recv1.at[j, pl.ds((4 + m) * h, h)], device)

    def sum_1(j):
        s, h = lax.rem(j, SUM_SLOTS), block // 2
        acc = own.at[lax.rem(j, OWN_SLOTS)]

        def keep(start, value):
            acc[pl.ds(start, value.shape[0])] = value
            sum1[s, pl.ds(start, value.shape[0])] = value.astype(jnp.bfloat16)

        def _direct():
            keep(0, added(j, 1, acc, recv1, p1, block))
            for m in range(3):
                sent(j, 1 + m, raw.at[0, pl.ds(0, block)])

        def _passed():
            for m in range(2, 6):
                got(j, 1 + m, recv1.at[j, pl.ds(m * h, h)])
            part = [recv1[j, pl.ds(m * h, h)].astype(jnp.float32) for m in range(2, 6)]
            upper = acc[rows(p1 * block, h)] + (part[1] + part[2])
            lower = acc[rows(p1 * block + h, h)] + (part[0] + part[3])
            keep(0, upper)
            keep(h, lower)
            for m in range(6):
                sent(j, 1 + m, mid1.at[0, 0])

        either(j, _direct, _passed)
        scatter(j, 7, sum1.at[s], recv2, p2, cell, far2, right2, left2)

    def cells(q1, q2):
        return core * half + q1 * block + q2 * cell

    def piece_rows(j, start, size):
        return res.at[j, rows(start, size)]

    def sum_2(j):
        acc = own.at[lax.rem(j, OWN_SLOTS)]
        res[j, rows(cells(p1, p2), cell)] = added(j, 7, acc, recv2, p2, cell).astype(jnp.bfloat16)
        mine = piece_rows(j, cells(p1, p2), cell)
        for m, device in enumerate((far2, right2, left2)):
            send(j, 13 + m, mine, mine, device)
        for m in range(3):
            sent(j, 7 + m, sum1.at[0, pl.ds(0, cell)])

    def gather_1(j):
        for m, by in enumerate((2, -1, 1)):
            got(j, 13 + m, piece_rows(j, cells(p1, step(p2, by)), cell))
        mine = piece_rows(j, cells(p1, 0), block)

        @pl.when(direct(j))
        def _():
            send(j, 19, mine, mine, far1)

        send(j, 17, mine, mine, right1)
        send(j, 18, mine, mine, left1)
        send(j, 21, mine, mine, partner)

    def gather_mid_1(j):
        h = block // 2
        from_left, from_right = cells(step(p1, -1), 0), cells(step(p1, 1), 0)
        got(j, 17, piece_rows(j, from_left, block))
        got(j, 18, piece_rows(j, from_right, block))

        @pl.when(jnp.logical_not(direct(j)))
        def _():
            upper, lower = piece_rows(j, from_left, h), piece_rows(j, from_right + h, h)
            send(j, 19, upper, upper, right1)
            send(j, 20, lower, lower, left1)

        for message, start in ((22, from_left), (23, from_right)):
            ref = piece_rows(j, start, block)
            send(j, message, ref, ref, partner)

    def gather_end(j):
        h, far = block // 2, cells(step(p1, 2), 0)

        def _passed():
            got(j, 19, piece_rows(j, far, h))
            got(j, 20, piece_rows(j, far + h, h))

        either(j, lambda: got(j, 19, piece_rows(j, far, block)), _passed)
        ref = piece_rows(j, far, block)
        send(j, 24, ref, ref, partner)

    def finish(j):
        whole, part = res.at[j, pl.ds(0, block)], res.at[j, pl.ds(0, block // 2)]
        for m in range(3):
            sent(j, 13 + m, res.at[j, pl.ds(0, cell)])
        for message in (17, 18, 21, 22, 23, 24):
            sent(j, message, whole)

        def _passed():
            sent(j, 19, part)
            sent(j, 20, part)

        either(j, lambda: sent(j, 19, whole), _passed)
        theirs = other * half
        for message, by in ((21, 0), (22, -1), (23, 1), (24, 2)):
            got(j, message, piece_rows(j, theirs + step(p2, by) * block, block))

    stages = {
        "own_half": own_half, "mid_1": mid_1, "sum_1": sum_1, "sum_2": sum_2, "gather_1": gather_1,
        "gather_mid_1": gather_mid_1, "gather_end": gather_end, "finish": finish,
    }

    def body(i, _):
        @pl.when((i >= 1) & (i < pieces))
        def _():
            partner_half(i)

        for part in range(2):
            todo = {}
            for is_direct, when in ((True, DIRECT), (False, PASSED)):
                for name, at_half in when.items():
                    if at_half % 2 == part:
                        todo.setdefault((at_half // 2, name), []).append(is_direct)
            order = sorted(todo, key=lambda k: (k[0], list(stages).index(k[1])))
            for late, name in order:
                j = i - late
                use = (j >= 0) & (j < pieces)
                if len(todo[late, name]) == 1:
                    mode = direct(j) if todo[late, name][0] else jnp.logical_not(direct(j))
                    use = use & mode
                pl.when(use)(functools.partial(stages[name], j))
        return 0

    last = max(max(when.values()) for when in (DIRECT, PASSED))
    lax.fori_loop(0, pieces + last // 2, body, 0)


def lay_out(pieces, width, res, out_hbm, sem):
    per_matrix = pieces // out_hbm.shape[0]
    copies = [
        pltpu.make_async_copy(
            res.at[j], out_hbm.at[j // per_matrix, :, pl.ds(j % per_matrix * width, width)], sem.at[j]
        )
        for j in range(pieces)
    ]
    for copy in copies:
        copy.start()
    for copy in copies:
        copy.wait()


def solution(mesh):
    devices = mesh.shape["dp"]
    assert devices == CORES * RING * RING and RING == math.isqrt(devices // CORES)

    def sums(a, g):
        _, matrices, tokens, d = a.shape
        ff = g.shape[3]
        width = 512 if ff % 512 == 0 else 128
        pieces = matrices * ff // width
        half = d // CORES
        block, cell = half // RING, half // RING // RING
        bf16, f32 = jnp.bfloat16, jnp.float32
        summed = pl.pallas_call(
            functools.partial(kernel, pieces, width),
            out_shape=pltpu.VMEM((pieces, d, width), bf16),
            in_specs=[pl.BlockSpec(memory_space=pltpu.HBM)] * 2,
            out_specs=pl.BlockSpec(memory_space=pltpu.VMEM),
            scratch_shapes=[
                pltpu.VMEM((matrices, 2, tokens, half), bf16),
                pltpu.VMEM((G_SLOTS, tokens, width), bf16),
                pltpu.VMEM((OWN_SLOTS, half, width), f32),
                pltpu.VMEM((2, half, width), bf16),
                pltpu.VMEM((pieces, half, width), bf16),
                pltpu.VMEM((RAW_SLOTS, half, width), bf16),
                pltpu.VMEM((MID_SLOTS, 2, block // 2, width), bf16),
                pltpu.VMEM((SUM_SLOTS, block, width), bf16),
                pltpu.VMEM((pieces, 3 * block, width), bf16),
                pltpu.VMEM((pieces, 3 * cell, width), bf16),
                pltpu.SemaphoreType.DMA((matrices, 2)),
                pltpu.SemaphoreType.DMA((pieces,)),
                pltpu.SemaphoreType.DMA((pieces, MESSAGES)),
                pltpu.SemaphoreType.DMA((pieces, MESSAGES)),
            ],
            compiler_params=pltpu.CompilerParams(
                collective_id=0, has_side_effects=True, vmem_limit_bytes=VMEM_BYTES
            ),
        )(a, g)
        return pl.pallas_call(
            functools.partial(lay_out, pieces, width),
            out_shape=jax.ShapeDtypeStruct((matrices, d, ff), bf16),
            in_specs=[pl.BlockSpec(memory_space=pl.ANY)],
            out_specs=pl.BlockSpec(memory_space=pltpu.HBM),
            scratch_shapes=[pltpu.SemaphoreType.DMA((pieces,))],
            compiler_params=pltpu.CompilerParams(vmem_limit_bytes=2**20),
        )(summed)

    spec = P(("rep", "dp"))
    return jax.shard_map(sums, mesh=mesh, in_specs=(spec, spec), out_specs=P("rep"), check_vma=False)
```

```python
import functools
import math

import jax
import jax.numpy as jnp
from jax import lax
from jax.experimental import pallas as pl
from jax.experimental.pallas import tpu as pltpu
from jax.sharding import PartitionSpec as P

CORES = 2
RING = 4
PAIR, UPPER, LOWER, BLOCKS, CELLS, OUT_CELLS, OUT_NEAR, OUT_FAR, HALF = range(9)
VMEM_BYTES = 52 * 2**20
MESH = pl.DeviceIdType.MESH

DIRECT_FIRST, DIRECT_LAST = 2, 2
GATHER_FIRST, GATHER_LAST = 2, 2
DIRECT = {"own_half": 3, "sum_1": 6, "sum_2": 9, "gather_1": 12, "gather_mid_1": 15, "gather_end": 15, "finish": 17}
PASSED = {"own_half": 3, "mid_1": 5, "sum_1": 8, "sum_2": 11, "gather_1": 14, "gather_mid_1": 17, "gather_end": 20, "finish": 22}


def slots(written, read):
    whens = [when for when in (DIRECT, PASSED) if written in when]
    return max((late[read] - early[written]) // 2 + 1 for late in whens for early in whens)


G_SLOTS = 3
OWN_SLOTS = slots("own_half", "sum_2")
RAW_SLOTS = slots("own_half", "sum_1")
MID_SLOTS = slots("mid_1", "sum_1")
SUM_SLOTS = slots("sum_1", "sum_2")


def kernel(
    pieces, width, a_hbm, g_hbm, res,
    a_buf, g_buf, own, pair_send, pair_recv, raw, mid1, sum1, recv1, recv2,
    a_sem, g_sem, send_sem, recv_sem,
):
    matrices, tokens, d = a_hbm.shape[1:]
    half = d // CORES
    block = half // RING
    cell = block // RING
    per_matrix = pieces // matrices

    me = lax.axis_index("dp")
    core = lax.rem(me, CORES)
    chip = me // CORES
    x, y = chip // RING, lax.rem(chip, RING)
    other = 1 - core
    p1 = x * other + y * core
    p2 = y * other + x * core

    def at(q1, q2):
        return ((q1 * other + q2 * core) * RING + q2 * other + q1 * core) * CORES + core

    def step(p, by):
        return lax.rem(p + by + RING, RING)

    partner = chip * CORES + other
    right1, left1, far1 = (at(step(p1, by), p2) for by in (1, -1, 2))
    right2, left2, far2 = (at(p1, step(p2, by)) for by in (1, -1, 2))
    peers = (partner, right1, left1, far1, right2, left2, far2)

    def rows(start, size):
        return pl.ds(pl.multiple_of(start, size), size)

    def copy(j, leaves, lands, src, dst, device):
        return pltpu.make_async_remote_copy(
            src_ref=src, dst_ref=dst, send_sem=send_sem.at[j, leaves], recv_sem=recv_sem.at[j, lands],
            device_id={"dp": device}, device_id_type=MESH,
        )

    def send(j, leaves, lands, src, dst, device):
        copy(j, leaves, lands, src, dst, device).start()

    def sent(j, leaves, ref):
        copy(j, leaves, leaves, ref, ref, partner).wait_send()

    def got(j, lands, ref):
        copy(j, lands, lands, ref, ref, partner).wait_recv()

    def load_a(n, h):
        start = (core * h + other * (1 - h)) * half
        return pltpu.make_async_copy(
            a_hbm.at[0, n, :, pl.ds(pl.multiple_of(start, half), half)], a_buf.at[n, h], a_sem.at[n, h]
        )

    def load_g(j):
        n, c = j // per_matrix, lax.rem(j, per_matrix)
        s = lax.rem(j, G_SLOTS)
        return pltpu.make_async_copy(
            g_hbm.at[0, n, :, pl.ds(pl.multiple_of(c * width, width), width)], g_buf.at[s], g_sem.at[j]
        )

    def dot(j, h):
        n, s = j // per_matrix, lax.rem(j, G_SLOTS)
        return lax.dot_general(
            a_buf[n, h], g_buf[s], (((0,), (0,)), ((), ())), preferred_element_type=jnp.float32
        )

    barrier = pltpu.get_barrier_semaphore()
    load_a(0, 0).start()
    load_g(0).start()
    for peer in peers:
        pl.semaphore_signal(barrier, inc=1, device_id={"dp": peer}, device_id_type=MESH)
    load_a(0, 1).start()
    load_g(1).start()
    load_g(2).start()

    def partner_dot(j):
        pair_send[lax.rem(j, 2)] = dot(j, 0).astype(jnp.bfloat16)

    def partner_send(j):
        send(j, PAIR, PAIR, pair_send.at[lax.rem(j, 2)], pair_recv.at[j], partner)

    load_g(0).wait()
    load_a(0, 0).wait()
    partner_dot(0)
    pl.semaphore_wait(barrier, len(peers))
    partner_send(0)

    def partner_half(j):
        load_g(j).wait()

        @pl.when(lax.rem(j, per_matrix) == 0)
        def _():
            load_a(j // per_matrix, 0).wait()

        @pl.when((lax.rem(j, per_matrix) == 1) & (j // per_matrix + 1 < matrices))
        def _():
            for h in range(2):
                load_a(j // per_matrix + 1, h).start()

        partner_dot(j)
        partner_send(j)

    def direct(j):
        return (j < DIRECT_FIRST) | (j >= pieces - DIRECT_LAST)

    def gathered_direct(j):
        return (j < GATHER_FIRST) | (j >= pieces - GATHER_LAST)

    def either(which, if_direct, if_passed):
        pl.when(which)(if_direct)
        pl.when(jnp.logical_not(which))(if_passed)

    def own_half(j):
        @pl.when(lax.rem(j, per_matrix) == 0)
        def _():
            load_a(j // per_matrix, 1).wait()

        s = lax.rem(j, RAW_SLOTS)
        got(j, PAIR, pair_recv.at[j])
        total = dot(j, 1) + pair_recv[j].astype(jnp.float32)
        own[lax.rem(j, OWN_SLOTS)] = total
        raw[s] = total.astype(jnp.bfloat16)

        @pl.when(j + G_SLOTS < pieces)
        def _():
            load_g(j + G_SLOTS).start()

        src, h = raw.at[s], block // 2
        far, near_r, near_l = (step(p1, by) * block for by in (2, 1, -1))

        def _direct():
            scatter(j, BLOCKS, src, recv1, p1, block, far1, right1, left1)

        def _passed():
            send(j, BLOCKS, UPPER, src.at[rows(far, h)], recv1.at[j, pl.ds(0, h)], right1)
            send(j, BLOCKS, LOWER, src.at[rows(far + h, h)], recv1.at[j, pl.ds(h, h)], left1)
            send(j, BLOCKS, BLOCKS, src.at[rows(near_r + h, h)], recv1.at[j, pl.ds(2 * h, h)], right1)
            send(j, BLOCKS, BLOCKS, src.at[rows(near_l, h)], recv1.at[j, pl.ds(3 * h, h)], left1)

        either(direct(j), _direct, _passed)
        sent(j, PAIR, pair_send.at[lax.rem(j, 2)])

    def scatter(j, group, src, dst, p, size, far, right, left):
        for m, (by, device) in enumerate(((2, far), (1, right), (-1, left))):
            part = src.at[rows(step(p, by) * size, size)]
            send(j, group, group, part, dst.at[j, pl.ds(m * size, size)], device)

    def added(j, group, acc, dst, p, size):
        got(j, group, dst.at[j])
        far, left, right = (dst[j, pl.ds(m * size, size)].astype(jnp.float32) for m in range(3))
        return acc[rows(p * size, size)] + (left + right + far)

    def mid_1(j):
        s, h = lax.rem(j, MID_SLOTS), block // 2
        acc = own.at[lax.rem(j, OWN_SLOTS)]
        for m, lands, device, start in (
            (0, UPPER, right1, step(p1, 1) * block), (1, LOWER, left1, step(p1, -1) * block + h)
        ):
            got(j, lands, recv1.at[j, pl.ds(m * h, h)])
            passed = acc[rows(start, h)] + recv1[j, pl.ds(m * h, h)].astype(jnp.float32)
            mid1[s, m] = passed.astype(jnp.bfloat16)
            send(j, BLOCKS, BLOCKS, mid1.at[s, m], recv1.at[j, pl.ds((4 + m) * h, h)], device)

    def sum_1(j):
        s, h = lax.rem(j, SUM_SLOTS), block // 2
        acc = own.at[lax.rem(j, OWN_SLOTS)]

        def keep(start, value):
            acc[pl.ds(start, value.shape[0])] = value
            sum1[s, pl.ds(start, value.shape[0])] = value.astype(jnp.bfloat16)

        def _direct():
            keep(0, added(j, BLOCKS, acc, recv1, p1, block))

        def _passed():
            got(j, BLOCKS, recv1.at[j, pl.ds(2 * h, 4 * h)])
            part = [recv1[j, pl.ds(m * h, h)].astype(jnp.float32) for m in range(2, 6)]
            upper = acc[rows(p1 * block, h)] + (part[1] + part[2])
            lower = acc[rows(p1 * block + h, h)] + (part[0] + part[3])
            keep(0, upper)
            keep(h, lower)

        either(direct(j), _direct, _passed)
        scatter(j, CELLS, sum1.at[s], recv2, p2, cell, far2, right2, left2)
        sent(j, BLOCKS, recv1.at[j])

    def cells(q1, q2):
        return core * half + q1 * block + q2 * cell

    def piece_rows(j, start, size):
        return res.at[j, rows(start, size)]

    def sum_2(j):
        acc = own.at[lax.rem(j, OWN_SLOTS)]
        res[j, rows(cells(p1, p2), cell)] = added(j, CELLS, acc, recv2, p2, cell).astype(jnp.bfloat16)
        mine = piece_rows(j, cells(p1, p2), cell)
        for device in (far2, right2, left2):
            send(j, HALF, OUT_CELLS, mine, mine, device)
        sent(j, CELLS, recv2.at[j])

    def gather_1(j):
        got(j, OUT_CELLS, res.at[j, pl.ds(0, 3 * cell)])
        mine = piece_rows(j, cells(p1, 0), block)

        @pl.when(gathered_direct(j))
        def _():
            send(j, HALF, OUT_FAR, mine, mine, far1)

        send(j, HALF, OUT_NEAR, mine, mine, right1)
        send(j, HALF, OUT_NEAR, mine, mine, left1)

    def gather_mid_1(j):
        h = block // 2
        got(j, OUT_NEAR, res.at[j, pl.ds(0, 2 * block)])

        @pl.when(jnp.logical_not(gathered_direct(j)))
        def _():
            upper = piece_rows(j, cells(step(p1, -1), 0), h)
            lower = piece_rows(j, cells(step(p1, 1), 0) + h, h)
            send(j, HALF, OUT_FAR, upper, upper, right1)
            send(j, HALF, OUT_FAR, lower, lower, left1)

    def gather_end(j):
        got(j, OUT_FAR, res.at[j, pl.ds(0, block)])
        ours = piece_rows(j, core * half, half)
        send(j, HALF, HALF, ours, ours, partner)

    def finish(j):
        got(j, HALF, piece_rows(j, other * half, half))
        sent(j, HALF, res.at[j, pl.ds(0, 3 * cell + 3 * block + half)])

    stages = {
        "own_half": own_half, "mid_1": mid_1, "sum_1": sum_1, "sum_2": sum_2, "gather_1": gather_1,
        "gather_mid_1": gather_mid_1, "gather_end": gather_end, "finish": finish,
    }

    def body(i, _):
        @pl.when((i >= 1) & (i < pieces))
        def _():
            partner_half(i)

        for part in range(2):
            todo = {}
            for is_direct, when in ((True, DIRECT), (False, PASSED)):
                for name, at_half in when.items():
                    if at_half % 2 == part:
                        todo.setdefault((at_half // 2, name), []).append(is_direct)
            order = sorted(todo, key=lambda k: (k[0], list(stages).index(k[1])))
            for late, name in order:
                j = i - late
                use = (j >= 0) & (j < pieces)
                if len(todo[late, name]) == 1:
                    mode = direct(j) if todo[late, name][0] else jnp.logical_not(direct(j))
                    use = use & mode
                pl.when(use)(functools.partial(stages[name], j))
        return 0

    last = max(max(when.values()) for when in (DIRECT, PASSED))
    lax.fori_loop(0, pieces + last // 2, body, 0)


def lay_out(pieces, width, res, out_hbm, sem):
    per_matrix = pieces // out_hbm.shape[0]
    copies = [
        pltpu.make_async_copy(
            res.at[j], out_hbm.at[j // per_matrix, :, pl.ds(j % per_matrix * width, width)], sem.at[j]
        )
        for j in range(pieces)
    ]
    for copy in copies:
        copy.start()
    for copy in copies:
        copy.wait()


def solution(mesh):
    devices = mesh.shape["dp"]
    assert devices == CORES * RING * RING and RING == math.isqrt(devices // CORES)

    def sums(a, g):
        _, matrices, tokens, d = a.shape
        ff = g.shape[3]
        width = 512 if ff % 512 == 0 else 128
        pieces = matrices * ff // width
        half = d // CORES
        block, cell = half // RING, half // RING // RING
        bf16, f32 = jnp.bfloat16, jnp.float32
        summed = pl.pallas_call(
            functools.partial(kernel, pieces, width),
            out_shape=pltpu.VMEM((pieces, d, width), bf16),
            in_specs=[pl.BlockSpec(memory_space=pltpu.HBM)] * 2,
            out_specs=pl.BlockSpec(memory_space=pltpu.VMEM),
            scratch_shapes=[
                pltpu.VMEM((matrices, 2, tokens, half), bf16),
                pltpu.VMEM((G_SLOTS, tokens, width), bf16),
                pltpu.VMEM((OWN_SLOTS, half, width), f32),
                pltpu.VMEM((2, half, width), bf16),
                pltpu.VMEM((pieces, half, width), bf16),
                pltpu.VMEM((RAW_SLOTS, half, width), bf16),
                pltpu.VMEM((MID_SLOTS, 2, block // 2, width), bf16),
                pltpu.VMEM((SUM_SLOTS, block, width), bf16),
                pltpu.VMEM((pieces, 3 * block, width), bf16),
                pltpu.VMEM((pieces, 3 * cell, width), bf16),
                pltpu.SemaphoreType.DMA((matrices, 2)),
                pltpu.SemaphoreType.DMA((pieces,)),
                pltpu.SemaphoreType.DMA((pieces, HALF + 1)),
                pltpu.SemaphoreType.DMA((pieces, HALF + 1)),
            ],
            compiler_params=pltpu.CompilerParams(
                collective_id=0, has_side_effects=True, vmem_limit_bytes=VMEM_BYTES
            ),
        )(a, g)
        return pl.pallas_call(
            functools.partial(lay_out, pieces, width),
            out_shape=jax.ShapeDtypeStruct((matrices, d, ff), bf16),
            in_specs=[pl.BlockSpec(memory_space=pl.ANY)],
            out_specs=pl.BlockSpec(memory_space=pltpu.HBM),
            scratch_shapes=[pltpu.SemaphoreType.DMA((pieces,))],
            compiler_params=pltpu.CompilerParams(vmem_limit_bytes=2**20),
        )(summed)

    spec = P(("rep", "dp"))
    return jax.shard_map(sums, mesh=mesh, in_specs=(spec, spec), out_specs=P("rep"), check_vma=False)
```

```python
import functools
import math

import jax
import jax.numpy as jnp
from jax import lax
from jax.experimental import pallas as pl
from jax.experimental.pallas import tpu as pltpu
from jax.sharding import PartitionSpec as P

CORES = 2
RING = 4
PAIR, UPPER, LOWER, BLOCKS, CELLS, OUT_CELLS, OUT_NEAR, OUT_FAR, HALF = range(9)
VMEM_BYTES = 52 * 2**20
MESH = pl.DeviceIdType.MESH

DIRECT_FIRST, DIRECT_LAST = 2, 2
GATHER_FIRST, GATHER_LAST = 2, 2
DIRECT = {"own_half": 3, "sum_1": 6, "sum_2": 9, "gather_1": 12, "gather_mid_1": 15, "gather_end": 15, "finish": 17}
PASSED = {"own_half": 3, "mid_1": 5, "sum_1": 8, "sum_2": 11, "gather_1": 14, "gather_mid_1": 17, "gather_end": 20, "finish": 22}


def slots(written, read):
    whens = [when for when in (DIRECT, PASSED) if written in when]
    return max((late[read] - early[written]) // 2 + 1 for late in whens for early in whens)


G_SLOTS = 3
OWN_SLOTS = slots("own_half", "sum_2")
RAW_SLOTS = slots("own_half", "sum_1")
MID_SLOTS = slots("mid_1", "sum_1")
SUM_SLOTS = slots("sum_1", "sum_2")


def kernel(
    pieces, width, a_hbm, g_hbm, res,
    a_buf, g_buf, own, pair_send, pair_recv, raw, mid1, sum1, recv1, recv2,
    a_sem, g_sem, first_sem, send_sem, recv_sem,
):
    matrices, tokens, d = a_hbm.shape[1:]
    half = d // CORES
    block = half // RING
    cell = block // RING
    per_matrix = pieces // matrices

    me = lax.axis_index("dp")
    core = lax.rem(me, CORES)
    chip = me // CORES
    x, y = chip // RING, lax.rem(chip, RING)
    other = 1 - core
    p1 = x * other + y * core
    p2 = y * other + x * core

    def at(q1, q2):
        return ((q1 * other + q2 * core) * RING + q2 * other + q1 * core) * CORES + core

    def step(p, by):
        return lax.rem(p + by + RING, RING)

    partner = chip * CORES + other
    right1, left1, far1 = (at(step(p1, by), p2) for by in (1, -1, 2))
    right2, left2, far2 = (at(p1, step(p2, by)) for by in (1, -1, 2))
    peers = (partner, right1, left1, far1, right2, left2, far2)

    def rows(start, size):
        return pl.ds(pl.multiple_of(start, size), size)

    def copy(j, leaves, lands, src, dst, device):
        return pltpu.make_async_remote_copy(
            src_ref=src, dst_ref=dst, send_sem=send_sem.at[j, leaves], recv_sem=recv_sem.at[j, lands],
            device_id={"dp": device}, device_id_type=MESH,
        )

    def send(j, leaves, lands, src, dst, device):
        copy(j, leaves, lands, src, dst, device).start()

    def sent(j, leaves, ref):
        copy(j, leaves, leaves, ref, ref, partner).wait_send()

    def got(j, lands, ref):
        copy(j, lands, lands, ref, ref, partner).wait_recv()

    def load_a(n, h):
        start = (core * h + other * (1 - h)) * half
        return pltpu.make_async_copy(
            a_hbm.at[0, n, :, pl.ds(pl.multiple_of(start, half), half)], a_buf.at[n, h], a_sem.at[n, h]
        )

    def load_g(j):
        n, c = j // per_matrix, lax.rem(j, per_matrix)
        s = lax.rem(j, G_SLOTS)
        return pltpu.make_async_copy(
            g_hbm.at[0, n, :, pl.ds(pl.multiple_of(c * width, width), width)], g_buf.at[s], g_sem.at[j]
        )

    some = tokens // 2

    def first_loads(k):
        part = pl.ds(k * some, some)
        columns = pl.ds(pl.multiple_of(other * half, half), half)
        return (
            pltpu.make_async_copy(a_hbm.at[0, 0, part, columns], a_buf.at[0, 0, part], first_sem.at[2 * k]),
            pltpu.make_async_copy(g_hbm.at[0, 0, part, pl.ds(0, width)], g_buf.at[0, part], first_sem.at[2 * k + 1]),
        )

    def dot(j, h, first=0, count=tokens):
        n, s = j // per_matrix, lax.rem(j, G_SLOTS)
        part = pl.ds(first, count)
        return lax.dot_general(
            a_buf[n, h, part], g_buf[s, part], (((0,), (0,)), ((), ())), preferred_element_type=jnp.float32
        )

    barrier = pltpu.get_barrier_semaphore()
    for k in range(2):
        for load in first_loads(k):
            load.start()
    for peer in peers:
        pl.semaphore_signal(barrier, inc=1, device_id={"dp": peer}, device_id_type=MESH)
    load_a(0, 1).start()
    load_g(1).start()
    load_g(2).start()

    def partner_dot(j):
        pair_send[lax.rem(j, 2)] = dot(j, 0).astype(jnp.bfloat16)

    def partner_send(j):
        send(j, PAIR, PAIR, pair_send.at[lax.rem(j, 2)], pair_recv.at[j], partner)

    for k in range(2):
        for load in first_loads(k):
            load.wait()
        value = dot(0, 0, k * some, some)
        if k == 0:
            own[0] = value
        else:
            pair_send[0] = (own[0] + value).astype(jnp.bfloat16)
    pl.semaphore_wait(barrier, len(peers))
    partner_send(0)

    def partner_half(j):
        load_g(j).wait()

        @pl.when(lax.rem(j, per_matrix) == 0)
        def _():
            load_a(j // per_matrix, 0).wait()

        @pl.when((lax.rem(j, per_matrix) == 1) & (j // per_matrix + 1 < matrices))
        def _():
            for h in range(2):
                load_a(j // per_matrix + 1, h).start()

        partner_dot(j)
        partner_send(j)

    def direct(j):
        return (j < DIRECT_FIRST) | (j >= pieces - DIRECT_LAST)

    def gathered_direct(j):
        return (j < GATHER_FIRST) | (j >= pieces - GATHER_LAST)

    def either(which, if_direct, if_passed):
        pl.when(which)(if_direct)
        pl.when(jnp.logical_not(which))(if_passed)

    def own_half(j):
        @pl.when(lax.rem(j, per_matrix) == 0)
        def _():
            load_a(j // per_matrix, 1).wait()

        s = lax.rem(j, RAW_SLOTS)
        got(j, PAIR, pair_recv.at[j])
        total = dot(j, 1) + pair_recv[j].astype(jnp.float32)
        own[lax.rem(j, OWN_SLOTS)] = total
        raw[s] = total.astype(jnp.bfloat16)

        @pl.when(j + G_SLOTS < pieces)
        def _():
            load_g(j + G_SLOTS).start()

        src, h = raw.at[s], block // 2
        far, near_r, near_l = (step(p1, by) * block for by in (2, 1, -1))

        def _direct():
            scatter(j, BLOCKS, src, recv1, p1, block, far1, right1, left1)

        def _passed():
            send(j, BLOCKS, UPPER, src.at[rows(far, h)], recv1.at[j, pl.ds(0, h)], right1)
            send(j, BLOCKS, LOWER, src.at[rows(far + h, h)], recv1.at[j, pl.ds(h, h)], left1)
            send(j, BLOCKS, BLOCKS, src.at[rows(near_r + h, h)], recv1.at[j, pl.ds(2 * h, h)], right1)
            send(j, BLOCKS, BLOCKS, src.at[rows(near_l, h)], recv1.at[j, pl.ds(3 * h, h)], left1)

        either(direct(j), _direct, _passed)
        sent(j, PAIR, pair_send.at[lax.rem(j, 2)])

    def scatter(j, group, src, dst, p, size, far, right, left):
        for m, (by, device) in enumerate(((2, far), (1, right), (-1, left))):
            part = src.at[rows(step(p, by) * size, size)]
            send(j, group, group, part, dst.at[j, pl.ds(m * size, size)], device)

    def added(j, group, acc, dst, p, size):
        got(j, group, dst.at[j])
        far, left, right = (dst[j, pl.ds(m * size, size)].astype(jnp.float32) for m in range(3))
        return acc[rows(p * size, size)] + (left + right + far)

    def mid_1(j):
        s, h = lax.rem(j, MID_SLOTS), block // 2
        acc = own.at[lax.rem(j, OWN_SLOTS)]
        for m, lands, device, start in (
            (0, UPPER, right1, step(p1, 1) * block), (1, LOWER, left1, step(p1, -1) * block + h)
        ):
            got(j, lands, recv1.at[j, pl.ds(m * h, h)])
            passed = acc[rows(start, h)] + recv1[j, pl.ds(m * h, h)].astype(jnp.float32)
            mid1[s, m] = passed.astype(jnp.bfloat16)
            send(j, BLOCKS, BLOCKS, mid1.at[s, m], recv1.at[j, pl.ds((4 + m) * h, h)], device)

    def sum_1(j):
        s, h = lax.rem(j, SUM_SLOTS), block // 2
        acc = own.at[lax.rem(j, OWN_SLOTS)]

        def keep(start, value):
            acc[pl.ds(start, value.shape[0])] = value
            sum1[s, pl.ds(start, value.shape[0])] = value.astype(jnp.bfloat16)

        def _direct():
            keep(0, added(j, BLOCKS, acc, recv1, p1, block))

        def _passed():
            got(j, BLOCKS, recv1.at[j, pl.ds(2 * h, 4 * h)])
            part = [recv1[j, pl.ds(m * h, h)].astype(jnp.float32) for m in range(2, 6)]
            upper = acc[rows(p1 * block, h)] + (part[1] + part[2])
            lower = acc[rows(p1 * block + h, h)] + (part[0] + part[3])
            keep(0, upper)
            keep(h, lower)

        either(direct(j), _direct, _passed)
        scatter(j, CELLS, sum1.at[s], recv2, p2, cell, far2, right2, left2)
        sent(j, BLOCKS, recv1.at[j])

    def cells(q1, q2):
        return core * half + q1 * block + q2 * cell

    def piece_rows(j, start, size):
        return res.at[j, rows(start, size)]

    def sum_2(j):
        acc = own.at[lax.rem(j, OWN_SLOTS)]
        res[j, rows(cells(p1, p2), cell)] = added(j, CELLS, acc, recv2, p2, cell).astype(jnp.bfloat16)
        mine = piece_rows(j, cells(p1, p2), cell)
        for device in (far2, right2, left2):
            send(j, HALF, OUT_CELLS, mine, mine, device)
        sent(j, CELLS, recv2.at[j])

    def gather_1(j):
        got(j, OUT_CELLS, res.at[j, pl.ds(0, 3 * cell)])
        mine = piece_rows(j, cells(p1, 0), block)

        @pl.when(gathered_direct(j))
        def _():
            send(j, HALF, OUT_FAR, mine, mine, far1)

        send(j, HALF, OUT_NEAR, mine, mine, right1)
        send(j, HALF, OUT_NEAR, mine, mine, left1)

    def gather_mid_1(j):
        h = block // 2
        got(j, OUT_NEAR, res.at[j, pl.ds(0, 2 * block)])

        @pl.when(jnp.logical_not(gathered_direct(j)))
        def _():
            upper = piece_rows(j, cells(step(p1, -1), 0), h)
            lower = piece_rows(j, cells(step(p1, 1), 0) + h, h)
            send(j, HALF, OUT_FAR, upper, upper, right1)
            send(j, HALF, OUT_FAR, lower, lower, left1)

    def gather_end(j):
        got(j, OUT_FAR, res.at[j, pl.ds(0, block)])
        ours = piece_rows(j, core * half, half)
        send(j, HALF, HALF, ours, ours, partner)

    def finish(j):
        got(j, HALF, piece_rows(j, other * half, half))
        sent(j, HALF, res.at[j, pl.ds(0, 3 * cell + 3 * block + half)])

    stages = {
        "own_half": own_half, "mid_1": mid_1, "sum_1": sum_1, "sum_2": sum_2, "gather_1": gather_1,
        "gather_mid_1": gather_mid_1, "gather_end": gather_end, "finish": finish,
    }

    def body(i, _):
        @pl.when((i >= 1) & (i < pieces))
        def _():
            partner_half(i)

        for part in range(2):
            todo = {}
            for is_direct, when in ((True, DIRECT), (False, PASSED)):
                for name, at_half in when.items():
                    if at_half % 2 == part:
                        todo.setdefault((at_half // 2, name), []).append(is_direct)
            order = sorted(todo, key=lambda k: (k[0], list(stages).index(k[1])))
            for late, name in order:
                j = i - late
                use = (j >= 0) & (j < pieces)
                if len(todo[late, name]) == 1:
                    mode = direct(j) if todo[late, name][0] else jnp.logical_not(direct(j))
                    use = use & mode
                pl.when(use)(functools.partial(stages[name], j))
        return 0

    last = max(max(when.values()) for when in (DIRECT, PASSED))
    lax.fori_loop(0, pieces + last // 2, body, 0)


def lay_out(pieces, width, res, out_hbm, sem):
    per_matrix = pieces // out_hbm.shape[0]
    copies = [
        pltpu.make_async_copy(
            res.at[j], out_hbm.at[j // per_matrix, :, pl.ds(j % per_matrix * width, width)], sem.at[j]
        )
        for j in range(pieces)
    ]
    for copy in copies:
        copy.start()
    for copy in copies:
        copy.wait()


def solution(mesh):
    devices = mesh.shape["dp"]
    assert devices == CORES * RING * RING and RING == math.isqrt(devices // CORES)

    def sums(a, g):
        _, matrices, tokens, d = a.shape
        ff = g.shape[3]
        width = 512 if ff % 512 == 0 else 128
        pieces = matrices * ff // width
        half = d // CORES
        block, cell = half // RING, half // RING // RING
        bf16, f32 = jnp.bfloat16, jnp.float32
        summed = pl.pallas_call(
            functools.partial(kernel, pieces, width),
            out_shape=pltpu.VMEM((pieces, d, width), bf16),
            in_specs=[pl.BlockSpec(memory_space=pltpu.HBM)] * 2,
            out_specs=pl.BlockSpec(memory_space=pltpu.VMEM),
            scratch_shapes=[
                pltpu.VMEM((matrices, 2, tokens, half), bf16),
                pltpu.VMEM((G_SLOTS, tokens, width), bf16),
                pltpu.VMEM((OWN_SLOTS, half, width), f32),
                pltpu.VMEM((2, half, width), bf16),
                pltpu.VMEM((pieces, half, width), bf16),
                pltpu.VMEM((RAW_SLOTS, half, width), bf16),
                pltpu.VMEM((MID_SLOTS, 2, block // 2, width), bf16),
                pltpu.VMEM((SUM_SLOTS, block, width), bf16),
                pltpu.VMEM((pieces, 3 * block, width), bf16),
                pltpu.VMEM((pieces, 3 * cell, width), bf16),
                pltpu.SemaphoreType.DMA((matrices, 2)),
                pltpu.SemaphoreType.DMA((pieces,)),
                pltpu.SemaphoreType.DMA((4,)),
                pltpu.SemaphoreType.DMA((pieces, HALF + 1)),
                pltpu.SemaphoreType.DMA((pieces, HALF + 1)),
            ],
            compiler_params=pltpu.CompilerParams(
                collective_id=0, has_side_effects=True, vmem_limit_bytes=VMEM_BYTES
            ),
        )(a, g)
        return pl.pallas_call(
            functools.partial(lay_out, pieces, width),
            out_shape=jax.ShapeDtypeStruct((matrices, d, ff), bf16),
            in_specs=[pl.BlockSpec(memory_space=pl.ANY)],
            out_specs=pl.BlockSpec(memory_space=pltpu.HBM),
            scratch_shapes=[pltpu.SemaphoreType.DMA((pieces,))],
            compiler_params=pltpu.CompilerParams(vmem_limit_bytes=2**20),
        )(summed)

    spec = P(("rep", "dp"))
    return jax.shard_map(sums, mesh=mesh, in_specs=(spec, spec), out_specs=P("rep"), check_vma=False)
```
